32 devices in a mesh: gx: 4 (over x, core), yz: 8 (over z, y).
Axes of the slice: x: 2, y: 2, z: 4, core: 2. Of those that a mesh axis runs over, the one named last changes fastest.
Arguments:
- fine_blocks: bfloat16 [256, 1536, 512], P(('gx', 'yz')), may hold values from -6 to 6
- fine_to_coarse: int32 [256], replicated, may hold values from 0 to 127, as said below
- widths: int32 [256], P(('gx', 'yz')), may hold values from 256 to 512
- pivots: int32 [128, 1024], P(('gx', 'yz')), may hold values from 0 to 1023, as said below
- neighbours: int32 [128, 4], P(('gx', 'yz')), may hold values from 0 to 3
Outputs:
- interp: float32 [128, 384, 640], P(('gx', 'yz'))
- schur_blocks: float32 [128, 384, 384], P(('gx', 'yz'))
The draws below stay inside these ranges and needn't reach their ends.
Inputs may be any that keep to these rules, and one draw needn't show every extreme that they name: `fine_to_coarse`: cluster c is owned by the device of index c // 4 along gx+yz, which has the same gx index as both its fine blocks; each cluster has exactly two fine blocks, on different devices, and the 8 blocks of one device belong to clusters of 8 different devices. `pivots`: each row is a permutation of 0 to 1023 whose first 384 entries are live columns (below the width of the first block, or 512 plus a column below the width of the second).
All inputs are finite; a program needn't handle non-finite values.
Results may differ from the reference program's by a relative error of at most 0.0003.
Values may be sent and summed in bfloat16 or wider, within the bound.
A program may use at most 192 MiB of HBM per device.

```python
import jax
import jax.numpy as jnp
from jax import lax

S = 512
K = 384
P_SIZE = 1536
FB_DEV = 8
NF = 256
NC = 128
W = 1024
N_GX = 4
N_YZ = 8


def child_pairs_drawn(mapping):
    count = mapping.shape[0]
    ids = jnp.arange(count, dtype=jnp.int32)
    earlier = (mapping[None, :] == mapping[:, None]) & (ids[None, :] < ids[:, None])
    earlier_count = jnp.sum(earlier.astype(jnp.int32), axis=1).astype(jnp.int32)
    child_slot = (2 * mapping + earlier_count).astype(jnp.int32)
    children = jnp.zeros((count,), jnp.int32).at[child_slot].set(ids)
    return children.reshape(count // 2, 2)


def plan_group(group_key):
    split_keys = jax.random.split(group_key, 5)
    relabel = jax.random.permutation(split_keys[0], N_YZ).astype(jnp.int32)
    spread = jax.random.permutation(split_keys[1], N_YZ).astype(jnp.int32)
    offsets = jax.random.permutation(split_keys[2], N_YZ).astype(jnp.int32)[:FB_DEV]
    block_order = jax.vmap(lambda sub_key: jax.random.permutation(sub_key, FB_DEV))(jax.random.split(split_keys[3], N_YZ)).astype(jnp.int32)
    pairing = jax.vmap(lambda sub_key: jax.random.permutation(sub_key, FB_DEV))(jax.random.split(split_keys[4], N_YZ)).astype(jnp.int32)
    sources = jnp.arange(N_YZ, dtype=jnp.int32)[:, None]
    target = relabel[(spread[sources] + offsets[block_order]) % N_YZ]
    return (target * (FB_DEV // 2) + pairing[target, block_order] // 2).astype(jnp.int32)


def routing(key):
    plans = jax.vmap(plan_group)(jax.random.split(jax.random.fold_in(key, 7), N_GX))
    groups = jnp.arange(N_GX, dtype=jnp.int32)[:, None, None]
    mapping = (groups * (N_YZ * (FB_DEV // 2)) + plans).reshape(NF).astype(jnp.int32)
    fine_widths = jax.random.randint(jax.random.fold_in(key, 9), (NF,), S // 2, S + 1, dtype=jnp.int32)
    children = child_pairs_drawn(mapping)
    width_first = fine_widths[children[:, 0]][:, None]
    width_second = fine_widths[children[:, 1]][:, None]
    col_ids = jnp.arange(W, dtype=jnp.int32)[None, :]
    live_cols = jnp.where(col_ids < S, col_ids < width_first, col_ids - S < width_second)
    ranks = jax.vmap(lambda sub_key: jax.random.permutation(sub_key, W))(jax.random.split(jax.random.fold_in(key, 13), NC)).astype(jnp.int32)
    scores = ranks + jnp.where(live_cols, 0, W).astype(jnp.int32)
    order = jnp.argsort(scores, axis=1, stable=True).astype(jnp.int32)
    return (mapping, fine_widths, order)


def draw_fine_to_coarse(key, part):
    return routing(key)[0]


def draw_widths(key, part):
    return routing(key)[1]


def draw_pivots(key, part):
    return routing(key)[2]


def set_ends(result, rng, low, top_value):
    place = [jax.random.randint(jax.random.fold_in(rng, axis), (), 0, length) for axis, length in enumerate(result.shape)]
    widest = result.shape.index(max(result.shape))
    next_to = place[:widest] + [(place[widest] + 1) % result.shape[widest]] + place[widest + 1:]
    return result.at[tuple(place)].set(low).at[tuple(next_to)].set(top_value)


def levels(rng, shape, shards, low, high):
    factor_of, own = 1.0, jax.random.fold_in(rng, 6)
    for dim, blocks in shards:
        heights = jnp.exp(jax.random.uniform(jax.random.fold_in(own, dim), (blocks,), jnp.float32, low / len(shards), high / len(shards)))
        factor_of = factor_of * jnp.repeat(heights, shape[dim] // blocks).reshape([-1 if axis == dim else 1 for axis in range(len(shape))])
    return factor_of


def normal_values(stream_key, extent, scale, bound, shards=(), held_as=jnp.bfloat16):
    values = jax.random.normal(stream_key, extent, jnp.float32) * scale
    if len(shards) > 0:
        values = levels(stream_key, extent, shards, -0.22, 0.18) * values
    return jnp.clip(values, min=-bound, max=bound).astype(held_as)


def setup_inputs(seed: int = 0) -> dict:
    key_of = jax.random.split(jax.random.key(seed), 6)
    fine_blocks = normal_values(key_of[0], (NF, P_SIZE, S), 1.0, 6.0, ((0, 32),))
    fine_to_coarse = draw_fine_to_coarse(jax.random.fold_in(key_of[5], 71), 0)
    widths = draw_widths(jax.random.fold_in(key_of[5], 71), 0)
    pivots = draw_pivots(jax.random.fold_in(key_of[5], 71), 0)
    neighbours = set_ends(jax.random.randint(key_of[4], (NC, 4), 0, FB_DEV // 2), jax.random.fold_in(key_of[4], 1), 0, (FB_DEV // 2) - 1).astype(jnp.int32)
    return dict(fine_blocks=fine_blocks, fine_to_coarse=fine_to_coarse, widths=widths, pivots=pivots, neighbours=neighbours)


def child_pairs(mapping):
    count = mapping.shape[0]
    ids = jnp.arange(count, dtype=jnp.int32)
    earlier = (mapping[None, :] == mapping[:, None]) & (ids[None, :] < ids[:, None])
    earlier_count = jnp.sum(earlier.astype(jnp.int32), axis=1).astype(jnp.int32)
    child_slot = (2 * mapping + earlier_count).astype(jnp.int32)
    children = jnp.zeros((count,), jnp.int32).at[child_slot].set(ids)
    return children.reshape(count // 2, 2)

def reference(fine_blocks, fine_to_coarse, widths, pivots, neighbours):
    block_count = fine_blocks.shape[0]
    cluster_count = block_count // 2
    per_device = FB_DEV // 2
    column = jnp.arange(S, dtype=jnp.int32)
    live_cols = (column[None, :] < widths[:, None]).astype(jnp.bfloat16)
    masked = fine_blocks * live_cols[:, None, :]
    children = child_pairs(fine_to_coarse)

    def one_cluster(cluster):
        left_block = masked[children[cluster, 0]]
        right_block = masked[children[cluster, 1]]
        merged = jnp.concatenate([left_block, right_block], axis=1)
        pivoted = jnp.take(merged, pivots[cluster], axis=1)
        gram_rows = jnp.dot(pivoted[:, :K].T.astype(jnp.float32), pivoted.astype(jnp.float32), preferred_element_type=jnp.float32)
        factor = jnp.linalg.cholesky(gram_rows[:, :K])
        half_solved = jax.scipy.linalg.solve_triangular(factor, gram_rows[:, K:], lower=True)
        interp = jax.scipy.linalg.solve_triangular(factor, half_solved, lower=True, trans=1)
        update = jnp.dot(interp, interp.T, precision=lax.Precision.HIGHEST)
        return (interp, update)
    interp, update = lax.map(one_cluster, jnp.arange(cluster_count, dtype=jnp.int32))
    update_grid = update.reshape(N_GX, N_YZ, per_device, K, K)
    padded = jnp.pad(update_grid, ((1, 1), (1, 1), (0, 0), (0, 0), (0, 0)))

    def gather_one(cluster):
        gx_pos = cluster // (N_YZ * per_device)
        yz_pos = cluster // per_device % N_YZ
        chosen = neighbours[cluster]
        terms = padded[gx_pos, yz_pos + 1, chosen[0]] + padded[gx_pos + 2, yz_pos + 1, chosen[1]]
        terms = terms + padded[gx_pos + 1, yz_pos, chosen[2]] + padded[gx_pos + 1, yz_pos + 2, chosen[3]]
        return update[cluster] + terms
    schur_blocks = lax.map(gather_one, jnp.arange(cluster_count, dtype=jnp.int32))
    return (interp, schur_blocks)
```

```python
import functools

import jax
import jax.numpy as jnp
from jax import lax
from jax.experimental import pallas as pl
from jax.experimental.pallas import tpu as pltpu
from jax.sharding import PartitionSpec as P

K = 384
TILE = 128
CHUNKS = 4
HIGHEST = lax.Precision.HIGHEST


def prep_kernel(slot_ref, width_ref, x_ref, o_ref):
    width = width_ref[slot_ref[pl.program_id(0)]]
    lane = lax.broadcasted_iota(jnp.int32, (1, x_ref.shape[2]), 1)
    live = (lane < width).astype(jnp.float32).astype(jnp.bfloat16)
    o_ref[0] = x_ref[0] * live


def pack_outgoing(fine_blocks, source_slot, widths, chunk, rows):
    peers = source_slot.shape[0]
    cols = fine_blocks.shape[2]
    return pl.pallas_call(
        prep_kernel,
        grid_spec=pltpu.PrefetchScalarGridSpec(
            num_scalar_prefetch=2,
            grid=(peers,),
            in_specs=[pl.BlockSpec((1, rows, cols), lambda i, slot, width: (slot[i], chunk, 0))],
            out_specs=pl.BlockSpec((1, rows, cols), lambda i, slot, width: (i, 0, 0)),
        ),
        out_shape=jax.ShapeDtypeStruct((peers, rows, cols), jnp.bfloat16),
        cost_estimate=pl.CostEstimate(
            flops=peers * rows * cols, bytes_accessed=4 * peers * rows * cols, transcendentals=0
        ),
        name=f"pack_{chunk}",
    )(source_slot, widths, fine_blocks)


def gram_kernel(has_prev, first_ref, second_ref, a_ref, b_ref, piv_ref, *refs):
    out_ref = refs[-1]
    cols = a_ref.shape[2]
    piv = piv_ref[0]
    source = lax.broadcasted_iota(jnp.int32, (cols, 2 * cols), 0)
    pick_a = (source == piv).astype(jnp.float32).astype(jnp.bfloat16)
    pick_b = (source + cols == piv).astype(jnp.float32).astype(jnp.bfloat16)
    pivoted = jnp.dot(a_ref[0], pick_a, preferred_element_type=jnp.float32)
    pivoted += jnp.dot(b_ref[0], pick_b, preferred_element_type=jnp.float32)
    pivoted = pivoted.astype(jnp.bfloat16)
    kept = out_ref.shape[1]
    part = lax.dot_general(
        pivoted[:, :kept], pivoted, (((0,), (0,)), ((), ())), preferred_element_type=jnp.float32
    )
    if has_prev:
        out_ref[0] = refs[0][0] + part
    else:
        out_ref[0] = part


def gram_chunk(arrived, first_src, second, pivots, prev, kept_cols):
    _, rows, cols = arrived.shape
    clusters, merged_cols = pivots.shape
    out_spec = pl.BlockSpec((1, kept_cols, merged_cols), lambda c, f, s: (c, 0, 0))
    in_specs = [
        pl.BlockSpec((1, rows, cols), lambda c, f, s: (f[c], 0, 0)),
        pl.BlockSpec((1, rows, cols), lambda c, f, s: (s[c], 0, 0)),
        pl.BlockSpec((1, 1, merged_cols), lambda c, f, s: (c, 0, 0)),
    ]
    operands = [arrived, arrived, pivots.reshape(clusters, 1, merged_cols)]
    aliases = {}
    if prev is not None:
        in_specs.append(out_spec)
        operands.append(prev)
        aliases = {5: 0}
    return pl.pallas_call(
        functools.partial(gram_kernel, prev is not None),
        grid_spec=pltpu.PrefetchScalarGridSpec(
            num_scalar_prefetch=2, grid=(clusters,), in_specs=in_specs, out_specs=out_spec
        ),
        out_shape=jax.ShapeDtypeStruct((clusters, kept_cols, merged_cols), jnp.float32),
        input_output_aliases=aliases,
        cost_estimate=pl.CostEstimate(
            flops=2 * clusters * rows * merged_cols * (merged_cols + kept_cols),
            bytes_accessed=clusters * (4 * rows * cols + 8 * kept_cols * merged_cols),
            transcendentals=0,
        ),
        name="gram_chunk",
    )(first_src, second, *operands)


def factor_kernel(g_ref, x_ref, u_ref, work, inv):
    clusters, kept, cols = g_ref.shape
    panels = kept // TILE
    lane = lax.broadcasted_iota(jnp.int32, (8, TILE), 1)

    def sweep(k, carry):
        is_k = lane == k
        for c in range(clusters):
            a = inv[c]
            row = jnp.broadcast_to(inv[c, pl.ds(k, 1), :], (8, TILE))
            pivot = jnp.take_along_axis(
                row, jnp.full((8, TILE), k, jnp.int32), axis=1, mode="promise_in_bounds"
            )
            col = jnp.take_along_axis(
                a, jnp.full((TILE, TILE), k, jnp.int32), axis=1, mode="promise_in_bounds"
            )
            scaled = (jnp.where(is_k, 1.0, row) / pivot)[:1]
            inv[c] = jnp.where(is_k[:1], 0.0, a) - col * scaled
            inv[c, pl.ds(k, 1), :] = scaled
        return carry

    for p in range(panels):
        src = g_ref if p == 0 else work
        here = slice(p * TILE, (p + 1) * TILE)
        lo = (p + 1) * TILE
        for c in range(clusters):
            inv[c] = src[c, here, here]
        lax.fori_loop(0, TILE, sweep, 0)
        last = p == panels - 1

        def eliminate(c, carry):
            row = jnp.dot(inv[c], src[c, here, lo:], precision=HIGHEST)
            for i in range(panels):
                rows = slice(i * TILE, (i + 1) * TILE)
                if i == p:
                    value = row
                else:
                    value = src[c, rows, lo:] - jnp.dot(src[c, rows, here], row, precision=HIGHEST)
                if last:
                    x_ref[c, rows, :] = value
                else:
                    work[c, rows, lo:] = value
            return carry

        lax.fori_loop(0, clusters, eliminate, 0)

    def outer(c, carry):
        slot = 0
        for i in range(panels):
            left = x_ref[c, i * TILE : (i + 1) * TILE, :]
            part = lax.dot_general(
                left,
                x_ref[c, : (i + 1) * TILE, :],
                (((1,), (1,)), ((), ())),
                precision=HIGHEST,
                preferred_element_type=jnp.float32,
            )
            for j in range(i + 1):
                u_ref[c, slot] = part[:, j * TILE : (j + 1) * TILE]
                slot += 1
        return carry

    lax.fori_loop(0, clusters, outer, 0)


def factor(gram):
    clusters, kept, cols = gram.shape
    panels = kept // TILE
    packed = panels * (panels + 1) // 2
    vmem = pl.BlockSpec(memory_space=pltpu.VMEM)
    return pl.pallas_call(
        factor_kernel,
        in_specs=[vmem],
        out_specs=[vmem, vmem],
        out_shape=[
            jax.ShapeDtypeStruct((clusters, kept, cols - kept), jnp.float32),
            jax.ShapeDtypeStruct((clusters, packed, TILE, TILE), jnp.float32),
        ],
        scratch_shapes=[
            pltpu.VMEM((clusters, kept, cols), jnp.float32),
            pltpu.VMEM((clusters, TILE, TILE), jnp.float32),
        ],
        name="factor",
    )(gram)


def combine_kernel(near_ref, own_ref, *refs):
    out_ref = refs[-1]
    panels = out_ref.shape[1] // TILE
    slot = 0
    for i in range(panels):
        for j in range(i + 1):
            total = own_ref[0, slot]
            for ref in refs[:-1]:
                total = total + ref[0, slot]
            rows = slice(i * TILE, (i + 1) * TILE)
            cols = slice(j * TILE, (j + 1) * TILE)
            out_ref[0, rows, cols] = total
            if i != j:
                out_ref[0, cols, rows] = total.T
            slot += 1


def combine(own, received, neighbours, kept):
    clusters, packed = own.shape[:2]
    block = (1, packed, TILE, TILE)

    def near_spec(side):
        return pl.BlockSpec(block, lambda c, near: (near[4 * c + side], 0, 0, 0))

    return pl.pallas_call(
        combine_kernel,
        grid_spec=pltpu.PrefetchScalarGridSpec(
            num_scalar_prefetch=1,
            grid=(clusters,),
            in_specs=[pl.BlockSpec(block, lambda c, near: (c, 0, 0, 0))]
            + [near_spec(side) for side in range(4)],
            out_specs=pl.BlockSpec((1, kept, kept), lambda c, near: (c, 0, 0)),
        ),
        out_shape=jax.ShapeDtypeStruct((clusters, kept, kept), jnp.float32),
        name="combine",
    )(neighbours.reshape(-1), own, *received)


def exchange(values):
    received = []
    for axis in ("gx", "yz"):
        ends = lax.axis_size(axis) - 1
        received.append(lax.ppermute(values, axis, [(i, i + 1) for i in range(ends)]))
        received.append(lax.ppermute(values, axis, [(i + 1, i) for i in range(ends)]))
    return received


def body(fine_blocks, fine_to_coarse, widths, pivots, neighbours):
    gx_count = lax.axis_size("gx")
    yz_count = lax.axis_size("yz")
    gx_pos = lax.axis_index("gx")
    yz_pos = lax.axis_index("yz")
    blocks_dev, depth, _ = fine_blocks.shape
    clusters = blocks_dev // 2
    device = gx_pos * yz_count + yz_pos
    cluster_table = fine_to_coarse.reshape(gx_count, yz_count, blocks_dev)
    grouped = lax.dynamic_index_in_dim(cluster_table, gx_pos, 0, keepdims=False)
    own_targets = lax.dynamic_index_in_dim(grouped, yz_pos, 0, keepdims=False)
    target = own_targets // clusters - gx_pos * yz_count
    peer_ids = jnp.arange(yz_count, dtype=jnp.int32)
    matches = target[None, :] == peer_ids[:, None]
    source_slot = jnp.sum(
        jnp.where(matches, jnp.arange(blocks_dev, dtype=jnp.int32)[None, :], 0), axis=1
    )
    owned_here = grouped // clusters == device
    member = jnp.any(
        owned_here[None] & ((grouped % clusters)[None] == jnp.arange(clusters)[:, None, None]),
        axis=2,
    )
    first_src = jnp.min(jnp.where(member, peer_ids[None, :], yz_count), axis=1)
    second = jnp.max(jnp.where(member, peer_ids[None, :], -1), axis=1)
    rows = depth // CHUNKS
    gram = None
    for chunk in range(CHUNKS):
        outgoing = pack_outgoing(fine_blocks, source_slot, widths, chunk, rows)
        arrived = lax.all_to_all(outgoing, "yz", split_axis=0, concat_axis=0, tiled=True)
        gram = gram_chunk(arrived, first_src, second, pivots, gram, K)
    interp, packed = factor(gram)
    schur_blocks = combine(packed, exchange(packed), neighbours, K)
    return (interp, schur_blocks)


def solution(mesh):
    return jax.shard_map(
        body,
        mesh=mesh,
        in_specs=(
            P(("gx", "yz"), None, None),
            P(),
            P(("gx", "yz")),
            P(("gx", "yz"), None),
            P(("gx", "yz"), None),
        ),
        out_specs=(P(("gx", "yz"), None, None), P(("gx", "yz"), None, None)),
        check_vma=False,
    )
```

```python
import functools

import jax
import jax.numpy as jnp
from jax import lax
from jax.experimental import pallas as pl
from jax.experimental.pallas import tpu as pltpu
from jax.sharding import PartitionSpec as P

K = 384
TILE = 128
CHUNKS = (1, 2, 1)
HIGHEST = lax.Precision.HIGHEST


def prep_kernel(slot_ref, width_ref, x_ref, o_ref):
    width = width_ref[slot_ref[pl.program_id(0)]]
    lane = lax.broadcasted_iota(jnp.int32, (1, x_ref.shape[2]), 1)
    live = (lane < width).astype(jnp.float32).astype(jnp.bfloat16)
    o_ref[0] = x_ref[0] * live


def pack_outgoing(fine_blocks, source_slot, widths, first, count, rows):
    peers = source_slot.shape[0]
    cols = fine_blocks.shape[2]
    total = peers * count * rows * cols
    return pl.pallas_call(
        prep_kernel,
        grid_spec=pltpu.PrefetchScalarGridSpec(
            num_scalar_prefetch=2,
            grid=(peers, count),
            in_specs=[
                pl.BlockSpec((1, rows, cols), lambda i, j, slot, width: (slot[i], first + j, 0))
            ],
            out_specs=pl.BlockSpec((1, rows, cols), lambda i, j, slot, width: (i, j, 0)),
        ),
        out_shape=jax.ShapeDtypeStruct((peers, count * rows, cols), jnp.bfloat16),
        cost_estimate=pl.CostEstimate(flops=total, bytes_accessed=4 * total, transcendentals=0),
        name=f"pack_{first}",
    )(source_slot, widths, fine_blocks)


def gram_kernel(has_prev, first_ref, second_ref, a_ref, b_ref, piv_ref, *refs):
    out_ref = refs[-1]
    cols = a_ref.shape[2]
    piv = piv_ref[0]
    source = lax.broadcasted_iota(jnp.int32, (cols, 2 * cols), 0)
    pick_a = (source == piv).astype(jnp.float32).astype(jnp.bfloat16)
    pick_b = (source + cols == piv).astype(jnp.float32).astype(jnp.bfloat16)
    pivoted = jnp.dot(a_ref[0], pick_a, preferred_element_type=jnp.float32)
    pivoted += jnp.dot(b_ref[0], pick_b, preferred_element_type=jnp.float32)
    pivoted = pivoted.astype(jnp.bfloat16)
    kept = out_ref.shape[1]
    part = lax.dot_general(
        pivoted[:, :kept], pivoted, (((0,), (0,)), ((), ())), preferred_element_type=jnp.float32
    )
    if has_prev:
        out_ref[0] = refs[0][0] + part
    else:
        out_ref[0] = part


def gram_chunk(arrived, first_src, second, pivots, prev, kept_cols):
    _, rows, cols = arrived.shape
    clusters, merged_cols = pivots.shape
    out_spec = pl.BlockSpec((1, kept_cols, merged_cols), lambda c, f, s: (c, 0, 0))
    in_specs = [
        pl.BlockSpec((1, rows, cols), lambda c, f, s: (f[c], 0, 0)),
        pl.BlockSpec((1, rows, cols), lambda c, f, s: (s[c], 0, 0)),
        pl.BlockSpec((1, 1, merged_cols), lambda c, f, s: (c, 0, 0)),
    ]
    operands = [arrived, arrived, pivots.reshape(clusters, 1, merged_cols)]
    aliases = {}
    if prev is not None:
        in_specs.append(out_spec)
        operands.append(prev)
        aliases = {5: 0}
    return pl.pallas_call(
        functools.partial(gram_kernel, prev is not None),
        grid_spec=pltpu.PrefetchScalarGridSpec(
            num_scalar_prefetch=2, grid=(clusters,), in_specs=in_specs, out_specs=out_spec
        ),
        out_shape=jax.ShapeDtypeStruct((clusters, kept_cols, merged_cols), jnp.float32),
        input_output_aliases=aliases,
        cost_estimate=pl.CostEstimate(
            flops=2 * clusters * rows * merged_cols * (merged_cols + kept_cols),
            bytes_accessed=clusters * (4 * rows * cols + 8 * kept_cols * merged_cols),
            transcendentals=0,
        ),
        name="gram_chunk",
    )(first_src, second, *operands)


def factor_kernel(g_ref, x_ref, u_ref, work, inv):
    clusters, kept, cols = g_ref.shape
    panels = kept // TILE
    sub = TILE // clusters
    lane = lax.broadcasted_iota(jnp.int32, (sub, TILE), 1)
    row_id = lax.broadcasted_iota(jnp.int32, (sub, TILE), 0)
    segment = lane // sub
    offset = lane - segment * sub
    wide_segment = lax.broadcasted_iota(jnp.int32, (TILE, TILE), 1) // sub

    def invert_small(a):
        for k in range(sub):
            index = segment * sub + k
            col = jnp.take_along_axis(a, index, axis=1, mode="promise_in_bounds")
            row = jnp.broadcast_to(a[k : k + 1, :], (sub, TILE))
            pivot = jnp.broadcast_to(col[k : k + 1, :], (sub, TILE))
            is_k = offset == k
            scaled = jnp.where(is_k, 1.0, row) / pivot
            a = jnp.where(row_id == k, scaled, jnp.where(is_k, 0.0, a) - col * scaled)
        return a

    def invert_block(q):
        here = slice(q * sub, (q + 1) * sub)
        small = jnp.zeros((sub, TILE), jnp.float32)
        for c in range(clusters):
            moved = inv[c, here, :]
            if c != q:
                moved = pltpu.roll(moved, ((c - q) * sub) % TILE, 1)
            small = jnp.where(segment == c, moved, small)
        small = invert_small(small)
        for c in range(clusters):
            block = inv[c]
            moved = small
            if c != q:
                moved = pltpu.roll(small, ((q - c) * sub) % TILE, 1)
            pivot_inv = jnp.where(segment == q, moved, 0.0)
            row = jnp.dot(pivot_inv, block, precision=HIGHEST)
            row = jnp.where(segment == q, moved, row)
            parts = [row]
            if q > 0:
                parts.insert(0, jnp.zeros((q * sub, TILE), jnp.float32))
            if q < clusters - 1:
                parts.append(jnp.zeros(((clusters - 1 - q) * sub, TILE), jnp.float32))
            padded = jnp.concatenate(parts, axis=0)
            in_q = wide_segment == q
            step = jnp.dot(jnp.where(in_q, block, 0.0), padded, precision=HIGHEST)
            inv[c] = jnp.where(in_q, 0.0, block) - step
            inv[c, here, :] = row

    for p in range(panels):
        src = g_ref if p == 0 else work
        here = slice(p * TILE, (p + 1) * TILE)
        lo = (p + 1) * TILE
        for c in range(clusters):
            inv[c] = src[c, here, here]
        for q in range(clusters):
            invert_block(q)
        last = p == panels - 1

        def eliminate(c, carry):
            row = jnp.dot(inv[c], src[c, here, lo:], precision=HIGHEST)
            for i in range(panels):
                rows = slice(i * TILE, (i + 1) * TILE)
                if i == p:
                    value = row
                else:
                    value = src[c, rows, lo:] - jnp.dot(src[c, rows, here], row, precision=HIGHEST)
                if last:
                    x_ref[c, rows, :] = value
                else:
                    work[c, rows, lo:] = value
            return carry

        lax.fori_loop(0, clusters, eliminate, 0)

    def outer(c, carry):
        slot = 0
        for i in range(panels):
            left = x_ref[c, i * TILE : (i + 1) * TILE, :]
            part = lax.dot_general(
                left,
                x_ref[c, : (i + 1) * TILE, :],
                (((1,), (1,)), ((), ())),
                precision=HIGHEST,
                preferred_element_type=jnp.float32,
            )
            for j in range(i + 1):
                u_ref[c, slot] = part[:, j * TILE : (j + 1) * TILE]
                slot += 1
        return carry

    lax.fori_loop(0, clusters, outer, 0)


def factor(gram):
    clusters, kept, cols = gram.shape
    panels = kept // TILE
    packed = panels * (panels + 1) // 2
    vmem = pl.BlockSpec(memory_space=pltpu.VMEM)
    return pl.pallas_call(
        factor_kernel,
        in_specs=[vmem],
        out_specs=[vmem, vmem],
        out_shape=[
            jax.ShapeDtypeStruct((clusters, kept, cols - kept), jnp.float32),
            jax.ShapeDtypeStruct((clusters, packed, TILE, TILE), jnp.float32),
        ],
        scratch_shapes=[
            pltpu.VMEM((clusters, kept, cols), jnp.float32),
            pltpu.VMEM((clusters, TILE, TILE), jnp.float32),
        ],
        name="factor",
    )(gram)


def combine_kernel(near_ref, own_ref, *refs):
    out_ref = refs[-1]
    panels = out_ref.shape[1] // TILE
    slot = 0
    for i in range(panels):
        for j in range(i + 1):
            total = own_ref[0, slot]
            for ref in refs[:-1]:
                total = total + ref[0, slot]
            rows = slice(i * TILE, (i + 1) * TILE)
            cols = slice(j * TILE, (j + 1) * TILE)
            out_ref[0, rows, cols] = total
            if i != j:
                out_ref[0, cols, rows] = total.T
            slot += 1


def combine(own, received, neighbours, kept):
    clusters, packed = own.shape[:2]
    block = (1, packed, TILE, TILE)

    def near_spec(side):
        return pl.BlockSpec(block, lambda c, near: (near[4 * c + side], 0, 0, 0))

    return pl.pallas_call(
        combine_kernel,
        grid_spec=pltpu.PrefetchScalarGridSpec(
            num_scalar_prefetch=1,
            grid=(clusters,),
            in_specs=[pl.BlockSpec(block, lambda c, near: (c, 0, 0, 0))]
            + [near_spec(side) for side in range(4)],
            out_specs=pl.BlockSpec((1, kept, kept), lambda c, near: (c, 0, 0)),
        ),
        out_shape=jax.ShapeDtypeStruct((clusters, kept, kept), jnp.float32),
        name="combine",
    )(neighbours.reshape(-1), own, *received)


def exchange(values):
    received = []
    for axis in ("gx", "yz"):
        ends = lax.axis_size(axis) - 1
        received.append(lax.ppermute(values, axis, [(i, i + 1) for i in range(ends)]))
        received.append(lax.ppermute(values, axis, [(i + 1, i) for i in range(ends)]))
    return received


def body(fine_blocks, fine_to_coarse, widths, pivots, neighbours):
    gx_count = lax.axis_size("gx")
    yz_count = lax.axis_size("yz")
    gx_pos = lax.axis_index("gx")
    yz_pos = lax.axis_index("yz")
    blocks_dev, depth, _ = fine_blocks.shape
    clusters = blocks_dev // 2
    device = gx_pos * yz_count + yz_pos
    cluster_table = fine_to_coarse.reshape(gx_count, yz_count, blocks_dev)
    grouped = lax.dynamic_index_in_dim(cluster_table, gx_pos, 0, keepdims=False)
    own_targets = lax.dynamic_index_in_dim(grouped, yz_pos, 0, keepdims=False)
    target = own_targets // clusters - gx_pos * yz_count
    peer_ids = jnp.arange(yz_count, dtype=jnp.int32)
    matches = target[None, :] == peer_ids[:, None]
    source_slot = jnp.sum(
        jnp.where(matches, jnp.arange(blocks_dev, dtype=jnp.int32)[None, :], 0), axis=1
    )
    owned_here = grouped // clusters == device
    member = jnp.any(
        owned_here[None] & ((grouped % clusters)[None] == jnp.arange(clusters)[:, None, None]),
        axis=2,
    )
    first_src = jnp.min(jnp.where(member, peer_ids[None, :], yz_count), axis=1)
    second = jnp.max(jnp.where(member, peer_ids[None, :], -1), axis=1)
    rows = depth // sum(CHUNKS)
    gram = None
    first = 0
    for count in CHUNKS:
        outgoing = pack_outgoing(fine_blocks, source_slot, widths, first, count, rows)
        first += count
        arrived = lax.all_to_all(outgoing, "yz", split_axis=0, concat_axis=0, tiled=True)
        gram = gram_chunk(arrived, first_src, second, pivots, gram, K)
    interp, packed = factor(gram)
    schur_blocks = combine(packed, exchange(packed), neighbours, K)
    return (interp, schur_blocks)


def solution(mesh):
    return jax.shard_map(
        body,
        mesh=mesh,
        in_specs=(
            P(("gx", "yz"), None, None),
            P(),
            P(("gx", "yz")),
            P(("gx", "yz"), None),
            P(("gx", "yz"), None),
        ),
        out_specs=(P(("gx", "yz"), None, None), P(("gx", "yz"), None, None)),
        check_vma=False,
    )
```
